32 devices in a mesh: role: 2 (over x), dp: 4 (over y, core), ctx: 4 (over z).
Axes of the slice: x: 2, y: 2, z: 4, core: 2. Of those that a mesh axis runs over, the one named last changes fastest.
Arguments:
- teacher_states: bfloat16 [4, 512, 5120], P('dp', 'ctx'), may hold values from -50 to 50
- student_states: bfloat16 [4, 512, 3584], P('dp', 'ctx'), may hold values from -50 to 50
- teacher_gain: float32 [5120], replicated, may hold values from 0.25 to 1.75
- student_gain: float32 [3584], replicated, may hold values from 0.25 to 1.75
- mentor_output_weights: bfloat16 [4, 5120, 2048], P(None, None, 'ctx'), may hold values from -2 to 2
- student_heads: bfloat16 [4, 3584, 2048], P(None, None, 'ctx'), may hold values from -2 to 2
- segments: int32 [4, 512], P('dp', 'ctx'), may hold values from 0 to 7, never falling along the last dimension, each value on 1 to 256 neighbouring positions
- targets: int32 [4, 512, 4], P('dp', 'ctx'), may hold values from 0 to 2047
Outputs:
- grad_heads: float32 [4, 3584, 2048], P(None, ('role', 'dp'), 'ctx')
- frame_terms: float32 [2, 4, 512, 4], P('role', 'dp', 'ctx')
The draws below stay inside these ranges and needn't reach their ends.
All inputs are finite; a program needn't handle non-finite values.
Results may differ from the reference program's by a relative error of at most 0.0048.
Values may be sent and summed in bfloat16 or wider, within the bound.
A program may use at most 192 MiB of HBM per device.

```python
import math
import jax
import jax.numpy as jnp
import numpy as np
from jax import lax

DT = 5120
DS = 3584
CODE_ALPHABET = 2048
QUANTIZER_TOTAL = 4
ROW_DEV = 128
SEQUENCE_STEPS = 512
DOCS = 8
N_DP = 4


def states_draw(key, seed_tag, model_width):
    values = jnp.clip(jax.random.normal(jax.random.fold_in(key, seed_tag), (N_DP, SEQUENCE_STEPS, model_width), jnp.float32), -5.0, 5.0)
    return values.astype(jnp.bfloat16)


def heads_draw(key, seed_tag, model_width):
    values = jnp.clip(jax.random.normal(jax.random.fold_in(key, seed_tag), (QUANTIZER_TOTAL, model_width, CODE_ALPHABET), jnp.float32), -5.0, 5.0)
    values = values * (3.0 / math.sqrt(model_width))
    return values.astype(jnp.bfloat16)


def draw_teacher_states(key, part):
    return states_draw(key, 11, DT)


def draw_student_states(key, part):
    return states_draw(key, 21, DS)


def draw_mentor_output_weights(key, part):
    return heads_draw(key, 31, DT)


def draw_student_heads(key, part):
    return heads_draw(key, 41, DS)


def place_ends(drawn, stream_key, low, top_value):
    index_at = [jax.random.randint(jax.random.fold_in(stream_key, axis), (), 0, length) for axis, length in enumerate(drawn.shape)]
    widest = drawn.shape.index(max(drawn.shape))
    neighbour = index_at[:widest] + [(index_at[widest] + 1) % drawn.shape[widest]] + index_at[widest + 1:]
    return drawn.at[tuple(index_at)].set(low).at[tuple(neighbour)].set(top_value)


def length_profile(number_of, total, limit, skew):
    weights = [(1 << 20) // math.isqrt(grade ** skew) + 1 for grade in range(2, number_of + 1)]
    rest, holding = total - limit - (number_of - 1), [1] * (number_of - 1)
    while rest > 0:
        free = [i for i in range(number_of - 1) if holding[i] < limit]
        mass, remaining = sum([weights[i] for i in free]), rest
        for i in free:
            addition = min(limit - holding[i], max(1, remaining * weights[i] // mass), rest)
            holding[i] = holding[i] + addition
            rest = rest - addition
    return np.array([limit] + holding)


def ragged(own_key, number_of, total, bound, skew):
    if number_of == 2:
        one = jax.random.randint(own_key, (), max(1, total - bound), min(bound, total - 1) + 1)
        return jnp.stack([one, total - one])
    sizes = jnp.asarray(length_profile(number_of, total, bound, skew), jnp.int32)
    twos = (number_of - 1) // 2
    source_of, receiver = sizes[1:1 + 2 * twos:2], sizes[2:2 + 2 * twos:2]
    slack = jnp.minimum(source_of - 1, bound - receiver)
    moved = jax.random.randint(jax.random.fold_in(own_key, 1), (twos,), 0, 1 << 20) % (slack + 1)
    sizes = sizes.at[1:1 + 2 * twos:2].set(source_of - moved).at[2:2 + 2 * twos:2].set(receiver + moved)
    return sizes[jax.random.permutation(jax.random.fold_in(own_key, 2), number_of)]


def setup_inputs(seed: int = 0) -> dict:
    arg_keys = jax.random.split(jax.random.key(seed), 9)
    return {
        "teacher_states": draw_teacher_states(jax.random.fold_in(arg_keys[8], 71), 0),
        "student_states": draw_student_states(jax.random.fold_in(arg_keys[8], 71), 0),
        "teacher_gain": jnp.clip(1.0 + 0.15 * jax.random.normal(arg_keys[2], (DT,), jnp.float32), 0.25, 1.75),
        "student_gain": jnp.clip(1.0 + 0.15 * jax.random.normal(arg_keys[3], (DS,), jnp.float32), 0.25, 1.75),
        "mentor_output_weights": draw_mentor_output_weights(jax.random.fold_in(arg_keys[8], 71), 0),
        "student_heads": draw_student_heads(jax.random.fold_in(arg_keys[8], 71), 0),
        "segments": jax.vmap(lambda own: jnp.searchsorted(jnp.cumsum(ragged(own, DOCS, SEQUENCE_STEPS, 2 * ROW_DEV, 2)), jnp.arange(SEQUENCE_STEPS), side="right"))(jax.random.split(arg_keys[6], N_DP)).reshape((N_DP, SEQUENCE_STEPS)).astype(jnp.int32),
        "targets": place_ends(jax.random.randint(arg_keys[7], (N_DP, SEQUENCE_STEPS, QUANTIZER_TOTAL), 0, CODE_ALPHABET), jax.random.fold_in(arg_keys[7], 1), 0, CODE_ALPHABET - 1).astype(jnp.int32),
    }


epsilon = 1e-06
sharpness_divisor = 2.0
blend_ratio = 0.5

def normalize(states, gain):
    values = states.astype(jnp.float32)
    factor = lax.rsqrt(lax.optimization_barrier(jnp.mean(values * values, axis=-1, keepdims=True)) + epsilon)
    return (values * factor * gain.astype(jnp.float32)).astype(jnp.bfloat16)

def project_books(rows, heads):
    return jnp.stack([jnp.dot(rows, heads[book], preferred_element_type=jnp.float32) for book in range(QUANTIZER_TOTAL)], axis=1)

def reference(teacher_states, student_states, teacher_gain, student_gain, mentor_output_weights, student_heads, segments, targets):
    teacher_rows = []
    learner_sample_slab = []
    gradient = jnp.zeros((QUANTIZER_TOTAL, DS, CODE_ALPHABET), jnp.float32)
    for sequence in range(N_DP):
        picked_code_index = jax.nn.one_hot(targets[sequence], CODE_ALPHABET, dtype=jnp.float32)
        mentor_unit_scaled = normalize(teacher_states[sequence], teacher_gain)
        mentor_activations = project_books(mentor_unit_scaled, mentor_output_weights) / sharpness_divisor
        teacher_logp = mentor_activations - jax.nn.logsumexp(mentor_activations, axis=-1, keepdims=True)
        teacher_rows.append(-lax.optimization_barrier(jnp.sum(picked_code_index * teacher_logp, axis=-1)))
        teacher_sent = lax.optimization_barrier(teacher_logp.astype(jnp.bfloat16)).astype(jnp.float32)
        student_normed = normalize(student_states[sequence], student_gain)
        learner_activations = project_books(student_normed, student_heads)
        untempered_logdensity = learner_activations - jax.nn.logsumexp(learner_activations, axis=-1, keepdims=True)
        warmed_activations = learner_activations / sharpness_divisor
        warmed_logdensity = warmed_activations - jax.nn.logsumexp(warmed_activations, axis=-1, keepdims=True)
        mentor_distribution = jnp.exp(teacher_sent)
        kullback_gap = lax.optimization_barrier(jnp.sum(mentor_distribution * (teacher_sent - warmed_logdensity), axis=-1))
        mismatch_penalty = -lax.optimization_barrier(jnp.sum(picked_code_index * untempered_logdensity, axis=-1))
        learner_sample_slab.append(blend_ratio * sharpness_divisor * sharpness_divisor * kullback_gap + (1.0 - blend_ratio) * mismatch_penalty)
        members = (segments[sequence][None, :] == jnp.arange(DOCS, dtype=jnp.int32)[:, None]).astype(jnp.float32)
        counts = lax.optimization_barrier(jnp.sum(members, axis=1))
        row_sizes = jnp.dot(counts, members, precision=lax.Precision.HIGHEST)
        sample_importance = SEQUENCE_STEPS / (DOCS * row_sizes)
        gradient_scaling = sample_importance[:, None, None] * (blend_ratio * sharpness_divisor * (jnp.exp(warmed_logdensity) - mentor_distribution) + (1.0 - blend_ratio) * (jnp.exp(untempered_logdensity) - picked_code_index))
        gradient_scaling = gradient_scaling.astype(jnp.bfloat16)
        gradient = gradient + jnp.stack([lax.dot_general(student_normed, gradient_scaling[:, book], (((0,), (0,)), ((), ())), preferred_element_type=jnp.float32) for book in range(QUANTIZER_TOTAL)])
    frame_terms = jnp.stack([jnp.stack(teacher_rows), jnp.stack(learner_sample_slab)])
    return (gradient, frame_terms)
```

```python
import itertools

import jax
import jax.numpy as jnp
from jax import lax
from jax.sharding import PartitionSpec as P

epsilon = 1e-06
sharpness_divisor = 2.0
blend_ratio = 0.5


def normalize(states, gain):
    values = states.astype(jnp.float32)
    factor = lax.rsqrt(jnp.mean(values * values, axis=-1, keepdims=True) + epsilon)
    return (values * factor * gain).astype(jnp.bfloat16)


def near_first(block, axis):
    count = lax.axis_size(axis)
    blocks = [block]
    for step in range(1, count):
        pairs = [(source, (source + step) % count) for source in range(count)]
        blocks.append(lax.ppermute(block, axis, pairs))
    return blocks


def line_gather(block, axis):
    count = lax.axis_size(axis)
    rank = lax.axis_index(axis)
    upward = [(source, source + 1) for source in range(count - 1)]
    downward = [(source + 1, source) for source in range(count - 1)]
    rising, falling = [block], [block]
    for _ in range(1, count):
        rising.append(lax.ppermute(rising[-1], axis, upward))
        falling.append(lax.ppermute(falling[-1], axis, downward))
    blocks = [block]
    for step in range(1, count):
        blocks.append(jnp.where(rank >= step, rising[step], falling[count - step]))
    return jnp.concatenate(blocks, axis=0)


def on_device(
    teacher_states,
    student_states,
    teacher_gain,
    student_gain,
    mentor_output_weights,
    student_heads,
    segments,
    targets,
):
    books, _, columns = mentor_output_weights.shape
    ctx_count = lax.axis_size("ctx")
    role_count = lax.axis_size("role")
    dp_count = lax.axis_size("dp")
    inner = 2 if dp_count % 2 == 0 else 1
    outer = dp_count // inner
    ctx_rank = lax.axis_index("ctx")
    role_rank = lax.axis_index("role")
    dp_rank = lax.axis_index("dp")
    rows_here = teacher_states.shape[1]
    half = rows_here // role_count
    group = half * ctx_count
    features = student_heads.shape[1] // (role_count * dp_count)

    def moved(value, shift):
        dr, do, di = shift
        pairs = []
        for r, o, i in itertools.product(range(role_count), range(outer), range(inner)):
            target = ((r + dr) % role_count, (o + do) % outer, (i + di) % inner)
            pairs.append(
                (
                    r * dp_count + o * inner + i,
                    target[0] * dp_count + target[1] * inner + target[2],
                )
            )
        return lax.ppermute(value, ("role", "dp"), pairs)

    def own_half(value):
        return lax.dynamic_slice_in_dim(value, role_rank * half, half, axis=0)

    order = (ctx_rank - jnp.arange(ctx_count)) % ctx_count
    selector = order[:, None] == jnp.arange(ctx_count)[None, :]

    def reorder(value):
        picks = selector.reshape(selector.shape + (1,) * (value.ndim - 1))
        return jnp.sum(jnp.where(picks, value[None], jnp.zeros((), value.dtype)), axis=1)

    student_rows = line_gather(normalize(own_half(student_states[0]), student_gain), "ctx")
    teacher_rows = line_gather(normalize(own_half(teacher_states[0]), teacher_gain), "ctx")

    packed = jnp.concatenate([segments[0][:, None], targets[0]], axis=1).T
    everything = reorder(jnp.stack(near_first(packed, "ctx")))
    all_segments = everything[:, 0].reshape(-1)
    length = all_segments.shape[0]
    documents = 2 * ctx_count
    members = (all_segments[None, :] == jnp.arange(documents, dtype=jnp.int32)[:, None]).astype(
        jnp.float32
    )
    counts = jnp.sum(members, axis=1, keepdims=True)
    row_sizes = jnp.sum(counts * members, axis=0)
    weights = (length / (documents * row_sizes)).reshape(ctx_count, rows_here)
    my_weights = lax.dynamic_slice_in_dim(weights, role_rank * half, half, axis=1)
    my_weights = reorder(my_weights).reshape(group)
    my_targets = lax.dynamic_slice_in_dim(everything[:, 1:], role_rank * half, half, axis=2)
    my_targets = reorder(my_targets).transpose(1, 0, 2).reshape(books, group)
    my_targets = my_targets - ctx_rank * columns

    shifts = list(itertools.product(range(role_count), range(outer), range(inner)))
    slabs = jnp.stack(
        [
            student_rows[:, place * features : (place + 1) * features]
            for place in range(role_count * dp_count)
        ]
    )
    feature_blocks = {}
    outer_rank, inner_rank = dp_rank // inner, dp_rank % inner
    for shift in shifts:
        dr, do, di = shift
        place = (
            ((role_rank + dr) % role_count) * dp_count
            + ((outer_rank + do) % outer) * inner
            + (inner_rank + di) % inner
        )
        slab = lax.dynamic_index_in_dim(slabs, place, axis=0, keepdims=False)
        feature_blocks[shift] = slab if not any(shift) else moved(slab, shift)

    positions = jnp.arange(columns)
    hits = [positions[None, :] == my_targets[q][:, None] for q in range(books)]

    def exchange(stats):
        kinds = stats.shape[0]
        value = reorder(stats.reshape(kinds, ctx_count, half).transpose(1, 0, 2))
        value = jnp.stack(near_first(value, "ctx"))
        value = reorder(value.transpose(1, 0, 2, 3))
        return value.transpose(1, 2, 0, 3).reshape(ctx_count, kinds // books, books, group)

    student_logits = [
        jnp.dot(student_rows, student_heads[q], preferred_element_type=jnp.float32)
        for q in range(books)
    ]
    scaled = [
        jnp.dot(teacher_rows, mentor_output_weights[q], preferred_element_type=jnp.float32)
        / sharpness_divisor
        for q in range(books)
    ]

    peaks, sums, picked = [], [], []
    for q in range(books):
        peak = jnp.max(scaled[q], axis=1)
        peaks.append(peak)
        sums.append(jnp.sum(jnp.exp(scaled[q] - peak[:, None]), axis=1))
        picked.append(jnp.sum(jnp.where(hits[q], scaled[q], 0.0), axis=1))
    student_peaks, plain_sums, warm_sums, student_picked = [], [], [], []
    for q in range(books):
        peak = jnp.max(student_logits[q], axis=1)
        centered = student_logits[q] - peak[:, None]
        student_peaks.append(peak)
        plain_sums.append(jnp.sum(jnp.exp(centered), axis=1))
        warm_sums.append(jnp.sum(jnp.exp(centered / sharpness_divisor), axis=1))
        student_picked.append(jnp.sum(jnp.where(hits[q], student_logits[q], 0.0), axis=1))
    shared = exchange(
        jnp.stack(
            peaks + sums + picked + student_peaks + plain_sums + warm_sums + student_picked
        )
    )

    def log_total(peak, total, divisor):
        largest = jnp.max(peak, axis=0)
        parts = total * jnp.exp((peak - largest[None]) / divisor)
        return largest / divisor + jnp.log(jnp.sum(parts, axis=0))

    teacher_norm = log_total(shared[:, 0], shared[:, 1], 1.0)
    teacher_terms = teacher_norm - jnp.sum(shared[:, 2], axis=0)
    plain_norm = log_total(shared[:, 3], shared[:, 4], 1.0)
    warm_norm = log_total(shared[:, 3], shared[:, 5], sharpness_divisor)
    mismatch_penalty = plain_norm - jnp.sum(shared[:, 6], axis=0)

    slopes, gaps = [], []
    for q in range(books):
        teacher_logp = (scaled[q] - teacher_norm[q][:, None]).astype(jnp.bfloat16)
        teacher_logp = teacher_logp.astype(jnp.float32)
        mentor_distribution = jnp.exp(teacher_logp)
        warmed = student_logits[q] / sharpness_divisor - warm_norm[q][:, None]
        untempered = student_logits[q] - plain_norm[q][:, None]
        gaps.append(jnp.sum(mentor_distribution * (teacher_logp - warmed), axis=1))
        slope = my_weights[:, None] * (
            blend_ratio * sharpness_divisor * (jnp.exp(warmed) - mentor_distribution)
            + (1.0 - blend_ratio) * (jnp.exp(untempered) - hits[q].astype(jnp.float32))
        )
        slopes.append(slope.astype(jnp.bfloat16))
    own_slope = jnp.concatenate(slopes, axis=1)

    total = None
    slope_blocks = {}
    for dr, do in itertools.product(range(role_count), range(outer)):
        block = own_slope if not (dr or do) else moved(own_slope, (dr, do, 0))
        slope_blocks[(dr, do, 0)] = block
        for di in range(1, inner):
            slope_blocks[(dr, do, di)] = moved(block, (0, 0, di))
    for shift in shifts:
        part = lax.dot_general(
            feature_blocks[shift],
            slope_blocks[shift],
            (((0,), (0,)), ((), ())),
            preferred_element_type=jnp.float32,
        )
        total = part if total is None else total + part
    shares = jnp.stack([total[:, q * columns : (q + 1) * columns] for q in range(books)])

    gap_parts = jnp.stack(gaps).reshape(books, ctx_count, half)
    own_gap = gap_parts[:, 0]
    for step in range(1, ctx_count):
        pairs = [(source, (source - step) % ctx_count) for source in range(ctx_count)]
        own_gap = own_gap + lax.ppermute(gap_parts[:, step], "ctx", pairs)
    student_terms = (
        blend_ratio * sharpness_divisor * sharpness_divisor * own_gap
        + (1.0 - blend_ratio) * mismatch_penalty[:, :half]
    )
    both = jnp.stack([teacher_terms[:, :half], student_terms])
    swapped = jnp.stack(near_first(both, "role"))
    holders = (role_rank - jnp.arange(role_count)) % role_count
    swapped = jnp.sum(
        jnp.where(
            (holders[:, None] == jnp.arange(role_count)[None, :])[:, :, None, None, None],
            swapped[None],
            0.0,
        ),
        axis=1,
    )
    mine = lax.dynamic_index_in_dim(swapped, role_rank, axis=1, keepdims=False)
    frame_terms = mine.transpose(0, 2, 1).reshape(1, 1, rows_here, books)
    return (shares, frame_terms)


def solution(mesh):
    return jax.shard_map(
        on_device,
        mesh=mesh,
        in_specs=(
            P("dp", "ctx", None),
            P("dp", "ctx", None),
            P(),
            P(),
            P(None, None, "ctx"),
            P(None, None, "ctx"),
            P("dp", "ctx"),
            P("dp", "ctx", None),
        ),
        out_specs=(P(None, ("role", "dp"), "ctx"), P("role", "dp", "ctx", None)),
        check_vma=False,
    )
```
